256 devices in a mesh: gx: 16 (over y, x), gy: 8 (over z_lo, core), ma: 2 (over z_hi).
Axes of the slice: x: 4, y: 4, z: 8 (z_hi: 2, z_lo: 4; z = z_hi * 4 + z_lo), core: 2. Of those that a mesh axis runs over, the one named last changes fastest.
Arguments:
- alpha_fields: bfloat16 [80, 2, 1024, 2048], P('ma', None, 'gy', 'gx'), may hold values from -6 to 6
- member_perts: bfloat16 [80, 2, 1024, 2048], P('ma', None, 'gy', 'gx'), may hold values from -0.625 to 0.625
- band_widths: int32 [2], replicated, may hold values from 2 to 8
- lat_index: int32 [2048], P('gy'), may hold values from 0 to 1022, as said below
- lat_weight: float32 [2048], P('gy'), may hold values from 0 to 1
- lon_index: int32 [4096], P('gx'), may hold values from 0 to 2047, as said below
- lon_weight: float32 [4096], P('gx'), may hold values from 0 to 1
- innovation: float32 [2, 2048, 4096], P(None, 'gy', 'gx'), may hold values from -6 to 6
- obs_weight: float32 [2, 2048, 4096], P(None, 'gy', 'gx'), may hold values from 0.1 to 1
Outputs:
- increment: float32 [2, 2048, 4096], P(None, 'gy', 'gx')
- gradient: float32 [80, 2, 1024, 2048], P('ma', None, 'gy', 'gx')
The draws below stay inside these ranges and needn't reach their ends.
Inputs may be any that keep to these rules, and one draw needn't show every extreme that they name: lat_index[p] is p // 2 - 1 or p // 2, clamped to 0 .. 1022. lon_index[q] is q // 2 - 1 or q // 2, taken modulo 2048.
All inputs are finite; a program needn't handle non-finite values.
Results may differ from the reference program's by a relative error of at most 0.0003.
Values may be sent and summed in bfloat16 or wider, within the bound.
A program may use at most 128 MiB of HBM per device.

```python
import math
import jax
import jax.numpy as jnp
from jax import lax

MEM = 80
LEV = 2
HB = 8
NCLAT = 1024
NCLON = 2048
NFLAT = 2048
NFLON = 4096


def draw_lat_index(key, part):
    position = jnp.arange(NFLAT, dtype=jnp.int32)
    backward = jax.random.randint(key, (NFLAT,), 0, 2, dtype=jnp.int32)
    return jnp.clip(position // 2 - backward, 0, NCLAT - 2).astype(jnp.int32)


def draw_lon_index(key, part):
    position = jnp.arange(NFLON, dtype=jnp.int32)
    backward = jax.random.randint(key, (NFLON,), 0, 2, dtype=jnp.int32)
    return jnp.remainder(position // 2 - backward, NCLON).astype(jnp.int32)


def steps_of(own_key, dims, cuts, smallest, top_value):
    def one(dim, shards_of):
        heights = jax.random.uniform(jax.random.fold_in(jax.random.fold_in(own_key, 6), dim), (shards_of,), jnp.float32, smallest / len(cuts), top_value / len(cuts))
        return jnp.repeat(jnp.exp(heights), dims[dim] // shards_of).reshape((-1,) + (1,) * (len(dims) - dim - 1))

    gain = one(*cuts[0])
    for cut in cuts[1:]:
        gain = gain * one(*cut)
    return gain


def normal_values(rng, extent, width, limit, shards=(), kind=jnp.bfloat16):
    entries = width * jax.random.normal(rng, extent, jnp.float32)
    if shards:
        entries = entries * steps_of(rng, extent, shards, -0.22, 0.18)
    return jnp.clip(entries, -limit, limit).astype(kind)


def setup_inputs(seed: int = 0) -> dict:
    splits = jax.random.split(jax.random.key(seed), 10)
    return {
        "alpha_fields": normal_values(splits[0], (MEM, LEV, NCLAT, NCLON), 1.0, 6.0, ((0, 2), (2, 8), (3, 16))),
        "member_perts": normal_values(splits[1], (MEM, LEV, NCLAT, NCLON), MEM ** -0.5, 0.625, ((0, 2), (2, 8), (3, 16))),
        "band_widths": jax.random.randint(splits[2], (LEV,), 2, HB + 1).astype(jnp.int32),
        "lat_index": draw_lat_index(jax.random.fold_in(splits[9], 71), 0),
        "lat_weight": jnp.clip(1.0 * jax.random.uniform(splits[4], (NFLAT,), jnp.float32) ** steps_of(splits[4], (NFLAT,), ((0, 8),), -0.2, 0.2), 0.0, 1.0),
        "lon_index": draw_lon_index(jax.random.fold_in(splits[9], 71), 0),
        "lon_weight": jnp.clip(1.0 * jax.random.uniform(splits[6], (NFLON,), jnp.float32) ** steps_of(splits[6], (NFLON,), ((0, 16),), -0.2, 0.2), 0.0, 1.0),
        "innovation": normal_values(splits[7], (LEV, NFLAT, NFLON), 1.0, 6.0, ((1, 8), (2, 16)), jnp.float32),
        "obs_weight": jnp.clip(jnp.exp(math.log(1.0) - 2.3025851 * jax.random.uniform(splits[8], (LEV, NFLAT, NFLON), jnp.float32) ** steps_of(splits[8], (LEV, NFLAT, NFLON), ((1, 8), (2, 16)), -0.2, 0.2)), 0.1, 1.0),
    }


def tap_table(band_widths):
    tap_offsets = jnp.arange(-HB, HB + 1).astype(jnp.float32)
    spread = band_widths.astype(jnp.float32)[:, None]
    shapes = jnp.exp(-tap_offsets[None, :] ** 2 / (2.0 * spread * spread))
    return shapes / jnp.sqrt(lax.optimization_barrier(jnp.sum(shapes * shapes, axis=1, keepdims=True)))

def localize(source, filter_taps):
    along_lon = jnp.zeros_like(source)
    for tap_number in range(2 * HB + 1):
        along_lon = along_lon + filter_taps[:, tap_number, None, None] * jnp.roll(source, HB - tap_number, axis=2)
    padded = jnp.pad(along_lon, ((0, 0), (HB, HB), (0, 0)))
    result = jnp.zeros_like(source)
    for tap_number in range(2 * HB + 1):
        result = result + filter_taps[:, tap_number, None, None] * padded[:, tap_number:tap_number + NCLAT, :]
    return result

def reference(alpha_fields, member_perts, band_widths, lat_index, lat_weight, lon_index, lon_weight, innovation, obs_weight):
    filter_taps = tap_table(band_widths)

    def accumulate(running, member_pair):
        localized = localize(member_pair[0].astype(jnp.float32), filter_taps)
        return (running + member_pair[1].astype(jnp.float32) * localized, None)
    coarse_increment, unused = lax.scan(accumulate, jnp.zeros((LEV, NCLAT, NCLON), jnp.float32), (alpha_fields, member_perts))
    lat_next = (lat_index + 1).astype(jnp.int32)
    lon_next = jnp.remainder(lon_index + 1, NCLON).astype(jnp.int32)
    north_weight = lat_weight[None, :, None]
    east_weight = lon_weight[None, None, :]
    by_lat = (1.0 - north_weight) * coarse_increment[:, lat_index, :] + north_weight * coarse_increment[:, lat_next, :]
    increment = (1.0 - east_weight) * by_lat[:, :, lon_index] + east_weight * by_lat[:, :, lon_next]
    misfit = obs_weight * (increment - innovation)
    spread_lon = jnp.zeros((LEV, NFLAT, NCLON), jnp.float32)
    spread_lon = spread_lon.at[:, :, lon_index].add((1.0 - east_weight) * misfit)
    spread_lon = spread_lon.at[:, :, lon_next].add(east_weight * misfit)
    coarse_residual = jnp.zeros((LEV, NCLAT, NCLON), jnp.float32)
    coarse_residual = coarse_residual.at[:, lat_index, :].add((1.0 - north_weight) * spread_lon)
    coarse_residual = coarse_residual.at[:, lat_next, :].add(north_weight * spread_lon)

    def member_gradient(member_pair):
        product = member_pair[1].astype(jnp.float32) * coarse_residual
        return member_pair[0].astype(jnp.float32) + localize(product, filter_taps)
    gradient = lax.map(member_gradient, (alpha_fields, member_perts))
    return (increment, gradient)
```

```python
import functools

import jax
import jax.numpy as jnp
from jax import lax
from jax.experimental import pallas as pl
from jax.experimental.pallas import tpu as pltpu
from jax.sharding import PartitionSpec as P

HB = 8
TILE = 128
EXT = 144
FINE = 256
GROUP = 8
F32 = jnp.float32
BF16 = jnp.bfloat16
MESH = pl.DeviceIdType.MESH
FLOWS = ((1, 0), (-1, 0), (0, 1), (0, -1), (1, 1), (1, -1), (-1, 1), (-1, -1))


def iota(shape, dim):
    return lax.broadcasted_iota(jnp.int32, shape, dim)


def dot(a, b):
    return jnp.dot(a, b, preferred_element_type=F32)


def exact_dot(a, b):
    return jnp.dot(a, b, preferred_element_type=F32, precision=lax.Precision.HIGHEST)


def split(x):
    high = x.astype(BF16)
    return high, (x - high.astype(F32)).astype(BF16)


def taps_at(distance, width):
    spread = jnp.full((8, 128), width.astype(F32), F32)[:1]
    scale = 1.0 / (2.0 * spread * spread)
    offset = (iota((1, 128), 1) - HB).astype(F32)
    shape = jnp.where(iota((1, 128), 1) <= 2 * HB, jnp.exp(-offset * offset * scale), 0.0)
    norm = 1.0 / jnp.sqrt(jnp.sum(shape * shape, axis=1, keepdims=True))
    gap = distance.astype(F32)
    values = jnp.exp(-gap * gap * scale[:, :1]) * norm
    return jnp.where(jnp.abs(distance) <= HB, values, 0.0)


def lon_taps(level, width):
    row = iota((2 * TILE, TILE), 0)
    col = iota((2 * TILE, TILE), 1)
    first = (row & 15) < 8
    west = first if level == 0 else jnp.logical_not(first)
    place = jnp.where(row < TILE, row, jnp.where(west, (row & 7) - HB, TILE + (row & 7)))
    high, low = split(taps_at(place - col, width))
    return jnp.concatenate([high, low], axis=1)


def lat_taps(width):
    row = iota((TILE, 512), 0)
    col = iota((TILE, 512), 1)
    part = (col >= EXT).astype(jnp.int32) + (col >= 2 * EXT).astype(jnp.int32) + (col >= 3 * EXT).astype(jnp.int32)
    k = col - EXT * part
    place = jnp.where(k < TILE, k, jnp.where(k < TILE + HB, k - TILE - HB, k - HB))
    values = taps_at(place - row, width)
    high = values.astype(BF16).astype(F32)
    chosen = jnp.where(part == 2, values - high, jnp.where(part == 3, 0.0, high))
    return chosen.astype(BF16)


def stencil_t(relative, weight):
    cell = iota((FINE, FINE), 0)

    def ext(r):
        return jnp.where(r < 0, r + EXT - HB, jnp.where(r >= TILE, r + HB, r))

    near = jnp.where(cell == ext(relative), 1.0 - weight, 0.0)
    return near + jnp.where(cell == ext(relative + 1), weight, 0.0)


def image_mask(level, j):
    lane = iota((1, TILE), 1)
    start = (lane - 16 * j + (8 if level == 1 else 0)) & 127
    return jnp.where(start < 16, 1.0, 0.0).astype(BF16)


def half_masks():
    lane = iota((1, TILE), 1)
    first = jnp.where((lane & 15) < 8, 1.0, 0.0)
    return first.astype(BF16), (1.0 - first).astype(BF16)


def lat_stack(y):
    high, low = split(y)
    return jnp.concatenate([high, low, high, jnp.zeros((512 - 3 * EXT, TILE), BF16)], axis=0)


def sum_kernel(
    alpha_hbm, perts_hbm, width_ref, lat_i, lat_w, lon_i, lon_w, innov_hbm, weight_hbm,
    inc_out, res_out, edge_out, ph_out, pw_out, pe_out, lon_out, lat_out,
    alpha, perts, ah, ph, pick, apk, ppk, aw, ae, pw, pe, awh, aeh,
    acc, other, coarse, ce, hc, innov, wobs, inc, resm, sel, rows, hm, hs,
    load_sem, a_send, a_recv, p_send, p_recv, m_send, m_recv, c_send, c_recv, r_send, r_recv, out_sem,
):
    gx, gy, ma = lax.axis_index("gx"), lax.axis_index("gy"), lax.axis_index("ma")
    nx, ny = lax.axis_size("gx"), lax.axis_size("gy")
    chunks = alpha.shape[0] // GROUP
    east, west = lax.rem(gx + 1, nx), lax.rem(gx + nx - 1, nx)
    has_up, has_down = gy > 0, gy < ny - 1

    def device(dx, dy):
        return (gx if dx == 0 else (east if dx == 1 else west), gy + dy, ma)

    def guard(dy, body):
        if dy == 0:
            body()
        else:
            pl.when(has_down if dy == 1 else has_up)(body)

    def load(i, b):
        src, dst = ((alpha_hbm, alpha), (perts_hbm, perts))[i]
        rows = pl.ds(b * GROUP, GROUP)
        return pltpu.make_async_copy(src.at[rows], dst.at[rows], load_sem.at[i, b])

    for i in range(2):
        for b in range(chunks):
            load(i, b).start()
    fine_loads = [
        pltpu.make_async_copy(innov_hbm, innov, load_sem.at[2, 0]),
        pltpu.make_async_copy(weight_hbm, wobs, load_sem.at[2, 1]),
    ]
    for copy in fine_loads:
        copy.start()

    barrier = pltpu.get_barrier_semaphore()
    for dx, dy in FLOWS:
        guard(dy, functools.partial(
            pl.semaphore_signal, barrier, inc=1, device_id=device(dx, dy), device_id_type=MESH))
    partner = (gx, gy, 1 - ma)
    pl.semaphore_signal(barrier, inc=1, device_id=partner, device_id_type=MESH)

    row = iota((2 * TILE, 2 * TILE), 0)
    col = iota((2 * TILE, 2 * TILE), 1)
    lane, lev = col & 127, row >> 7
    src = row & 127
    for j in range(GROUP):
        target_e = (16 * j - 8 * lev + src - 120) & 127
        target_w = (16 * j + 8 - 8 * lev + src) & 127
        hit = jnp.where(
            col < TILE,
            jnp.where(src >= 120, (lane == target_e).astype(jnp.int32), 0),
            jnp.where(src < 8, (lane == target_w).astype(jnp.int32), 0),
        )
        pick[j] = hit.astype(F32).astype(BF16)

    def pack(i, fields, packed):
        def one(b, carry):
            load(i, b).wait()
            total = jnp.zeros((TILE, 2 * TILE), F32)
            for j in range(GROUP):
                m = b * GROUP + j
                total = total + dot(jnp.concatenate([fields[m, 0], fields[m, 1]], axis=1), pick[j])
            packed[0, b] = total[:, :TILE].astype(BF16)
            packed[1, b] = total[:, TILE:].astype(BF16)
            return carry

        lax.fori_loop(0, chunks, one, 0)

    def band_copy(f, b, fields, packed, rows_halo, blocks, block_rows, send, recv):
        dx, dy = FLOWS[f]
        edge = pl.ds(TILE - HB, HB) if dy == 1 else pl.ds(0, HB)
        land = pl.ds(0, HB) if dy == 1 else pl.ds(HB, HB)
        members = pl.ds(b * GROUP, GROUP)
        if dx == 0:
            src, dst = fields.at[members, :, edge], rows_halo.at[members, :, land]
        elif dy == 0:
            src, dst = packed.at[0 if dx == 1 else 1, b], blocks[0 if dx == 1 else 1].at[b]
        else:
            src = packed.at[0 if dx == 1 else 1, b, edge]
            dst = block_rows[0 if dx == 1 else 1].at[b, land]
        return pltpu.make_async_remote_copy(
            src_ref=src, dst_ref=dst, send_sem=send.at[f, b], recv_sem=recv.at[f, b],
            device_id=device(dx, dy), device_id_type=MESH)

    a_args = (alpha, apk, ah, (aw, ae), (awh, aeh), a_send, a_recv)
    p_args = (perts, ppk, ph, (pw.at[:, pl.ds(0, TILE)], pe.at[:, pl.ds(0, TILE)]),
              (pw.at[:, pl.ds(TILE, 16)], pe.at[:, pl.ds(TILE, 16)]), p_send, p_recv)

    def each_band(action, args):
        def one(b, carry):
            for f, (dx, dy) in enumerate(FLOWS):
                copy = band_copy(f, b, *args)
                if action == "start":
                    guard(dy, copy.start)
                elif action == "send":
                    guard(dy, copy.wait_send)
                else:
                    guard(-dy, copy.wait_recv)
            return carry

        lax.fori_loop(0, chunks, one, 0)

    pack(0, alpha, apk)
    pl.semaphore_wait(
        barrier, 3 + 3 * has_up.astype(jnp.int32) + 3 * has_down.astype(jnp.int32))
    each_band("start", a_args)

    def clear(first):
        land = pl.ds(0, HB) if first else pl.ds(HB, HB)
        far = pl.ds(TILE, HB) if first else pl.ds(TILE + HB, HB)
        ah[:, :, land] = jnp.zeros((ah.shape[0], 2, HB, TILE), BF16)
        ph[:, :, land] = jnp.zeros((ah.shape[0], 2, HB, TILE), BF16)
        for block in (awh, aeh):
            block[:, land] = jnp.zeros((chunks, HB, TILE), BF16)
        for block in (pw, pe):
            block[:, far] = jnp.zeros((chunks, HB, TILE), BF16)
        dy = 1 if first else -1
        for f, flow in enumerate(FLOWS):
            if flow[1] == dy:
                hc[f] = jnp.zeros((2, HB, TILE), F32)
                hs[f] = jnp.zeros((2, 16, FINE), F32)
        hm[0 if first else 1] = jnp.zeros((2, 16, TILE), F32)

    pl.when(gy == 0)(functools.partial(clear, True))
    pl.when(gy == ny - 1)(functools.partial(clear, False))

    for level in range(2):
        lon_out[level] = lon_taps(level, width_ref[level])
        lat_out[level] = lat_taps(width_ref[level])

    pack(1, perts, ppk)
    each_band("start", p_args)

    mask_a, mask_b = half_masks()

    def partner_copy(level):
        return pltpu.make_async_remote_copy(
            src_ref=acc.at[level], dst_ref=other.at[level], send_sem=m_send.at[level],
            recv_sem=m_recv.at[level], device_id=partner, device_id_type=MESH)

    for level in range(2):
        acc[level] = jnp.zeros((TILE, TILE), F32)

        def chunk(b, carry, level=level):
            if level == 0:
                for f, (dx, dy) in enumerate(FLOWS):
                    guard(-dy, band_copy(f, b, *a_args).wait_recv)
            west_b = jnp.concatenate([aw[b], awh[b]], axis=0)
            east_b = jnp.concatenate([ae[b], aeh[b]], axis=0)
            edges = west_b * mask_a + east_b * mask_b if level == 0 else east_b * mask_a + west_b * mask_b
            total = acc[level]
            for pair in range(GROUP // 2):
                stacks = []
                for j in (2 * pair, 2 * pair + 1):
                    m = b * GROUP + j
                    own = jnp.concatenate([alpha[m, level], ah[m, level]], axis=0)
                    lhs = jnp.concatenate([own, edges * image_mask(level, j)], axis=1)
                    wide = dot(lhs, lon_out[level])
                    stacks.append(lat_stack(wide[:, :TILE] + wide[:, TILE:]))
                z = dot(lat_out[level], jnp.concatenate(stacks, axis=1))
                m = b * GROUP + 2 * pair
                total = total + perts[m, level].astype(F32) * z[:, :TILE]
                total = total + perts[m + 1, level].astype(F32) * z[:, TILE:]
            acc[level] = total
            return carry

        lax.fori_loop(0, chunks, chunk, 0)
        partner_copy(level).start()

    lat_rel = lat_i[...] - gy * TILE
    lon_rel = lax.rem(lon_i[...] - gx * TILE + 1 + nx * TILE, nx * TILE) - 1
    mt = stencil_t(lat_rel, lat_w[...])
    nt = stencil_t(lon_rel, lon_w[...])
    m_map = mt.T
    n_map = nt.T
    zeros_top = jnp.zeros((TILE - HB, FINE), F32)
    top_t = jnp.concatenate([zeros_top, mt[TILE:TILE + HB]], axis=0)
    bottom_t = jnp.concatenate([mt[TILE + HB:EXT], zeros_top], axis=0)
    corner_map = jnp.concatenate([mt[:TILE], top_t, bottom_t], axis=0)

    for level in range(2):
        copy = partner_copy(level)
        copy.wait_recv()
        total = acc[level] + other[level]
        coarse[level] = total
        turned = total.T
        ce[0, level] = turned[TILE - HB:]
        ce[1, level] = turned[:HB]

    def coarse_copy(f):
        dx, dy = FLOWS[f]
        edge = pl.ds(TILE - HB, HB) if dy == 1 else pl.ds(0, HB)
        src = coarse.at[:, edge] if dx == 0 else ce.at[0 if dx == 1 else 1]
        return pltpu.make_async_remote_copy(
            src_ref=src, dst_ref=hc.at[f], send_sem=c_send.at[f], recv_sem=c_recv.at[f],
            device_id=device(dx, dy), device_id_type=MESH)

    for f, (dx, dy) in enumerate(FLOWS):
        guard(dy, coarse_copy(f).start)
    for copy in fine_loads:
        copy.wait()
    for f, (dx, dy) in enumerate(FLOWS):
        guard(-dy, coarse_copy(f).wait_recv)

    for level in range(2):
        framed = jnp.concatenate(
            [coarse[level], hc[2, level], hc[3, level], jnp.zeros((FINE - EXT, TILE), F32)], axis=0)
        by_lat = exact_dot(m_map, framed)
        sides = jnp.concatenate([
            jnp.concatenate([hc[0, level], hc[1, level]], axis=0),
            jnp.concatenate([hc[4, level], hc[6, level]], axis=0),
            jnp.concatenate([hc[5, level], hc[7, level]], axis=0)], axis=1)
        side_t = exact_dot(sides, corner_map)
        side = jnp.concatenate([side_t, jnp.zeros((TILE - 16, FINE), F32)], axis=0).T
        fine = exact_dot(jnp.concatenate([by_lat, side], axis=1), nt)
        inc[level] = fine
        misfit = wobs[level] * (fine - innov[level])
        lon_back = exact_dot(misfit, n_map[:, :TILE])
        chosen = jnp.concatenate([nt[:HB], nt[TILE:TILE + HB], nt[TILE - HB:TILE], nt[TILE + HB:EXT]], axis=0)
        chosen_t = lax.dot_general(
            chosen, misfit, (((1,), (1,)), ((), ())), precision=lax.Precision.HIGHEST,
            preferred_element_type=F32)
        restricted = exact_dot(mt[:EXT], lon_back)
        resm[level] = restricted
        turned = exact_dot(chosen_t, m_map)
        sel[0, level] = turned[16:32]
        sel[1, level] = turned[:16]
        sel[2, level] = jnp.concatenate([turned[8:16], turned[24:32]], axis=0)
        rows[0, level] = jnp.concatenate([restricted[TILE - HB:TILE], restricted[TILE + HB:EXT]], axis=0)
        rows[1, level] = jnp.concatenate([restricted[:HB], restricted[TILE:TILE + HB]], axis=0)

    def edge_copies(f):
        dx, dy = FLOWS[f]
        copies = [pltpu.make_async_remote_copy(
            src_ref=sel.at[2 if dx == 0 else (0 if dx == 1 else 1)], dst_ref=hs.at[f],
            send_sem=r_send.at[f], recv_sem=r_recv.at[f],
            device_id=device(dx, dy), device_id_type=MESH)]
        if dx == 0:
            k = 0 if dy == 1 else 1
            copies.append(pltpu.make_async_remote_copy(
                src_ref=rows.at[k], dst_ref=hm.at[k], send_sem=r_send.at[8 + k], recv_sem=r_recv.at[8 + k],
                device_id=device(dx, dy), device_id_type=MESH))
        return copies

    for f, (dx, dy) in enumerate(FLOWS):
        for copy in edge_copies(f):
            guard(dy, copy.start)
    each_band("recv", p_args)
    results = [
        pltpu.make_async_copy(inc, inc_out, out_sem.at[0]),
        pltpu.make_async_copy(ph, ph_out, out_sem.at[1]),
        pltpu.make_async_copy(pw, pw_out, out_sem.at[2]),
        pltpu.make_async_copy(pe, pe_out, out_sem.at[3]),
    ]
    for copy in results:
        copy.start()
    for f, (dx, dy) in enumerate(FLOWS):
        for copy in edge_copies(f):
            guard(-dy, copy.wait_recv)

    lane = iota((32, FINE), 1)

    def joined(from_west, centre, from_east):
        halo = centre + jnp.concatenate([from_west[:HB], from_east[:HB]], axis=0)
        return jnp.concatenate([halo, from_west[HB:], from_east[HB:]], axis=0)

    def pick_lanes(x, first, first_shift, second, second_shift):
        a = pltpu.roll(x, first_shift, 1)
        b = pltpu.roll(x, second_shift, 1)
        in_a = (lane >= first) & (lane < first + HB)
        in_b = (lane >= second) & (lane < second + HB)
        return jnp.where(in_a, a, jnp.where(in_b, b, 0.0))

    for level in range(2):
        side = joined(hs[0, level], sel[2, level], hs[1, level])
        above = joined(hs[4, level], hs[2, level], hs[6, level])
        below = joined(hs[5, level], hs[3, level], hs[7, level])
        side = side + pick_lanes(above, TILE, 8, 0, 120)
        side = side + pick_lanes(below, TILE + HB, 136, TILE - HB, 248)
        turned = jnp.concatenate([side, jnp.zeros((TILE - 32, FINE), F32)], axis=0).T
        r = iota((TILE, FINE), 0)
        c = iota((TILE, FINE), 1)
        band = (c & 15) if level == 0 else (c & 15) ^ 8
        own = jnp.where(c < HB, c + 16, jnp.where(c >= TILE - HB, c - 96, -1))
        place = jnp.where(r == jnp.where(c < TILE, own, band), 1.0, 0.0)
        spread = exact_dot(turned, place)
        edge_out[level] = spread[:EXT, TILE:]
        top, bottom = hm[0, level], hm[1, level]
        gap = jnp.zeros((TILE - 2 * HB, TILE), F32)
        arrived = jnp.concatenate([top[HB:], gap, bottom[HB:], top[:HB], bottom[:HB]], axis=0)
        res_out[level] = resm[level] + spread[:EXT, :TILE] + arrived

    each_band("send", a_args)
    each_band("send", p_args)
    for level in range(2):
        partner_copy(level).wait_send()
    for f, (dx, dy) in enumerate(FLOWS):
        guard(dy, coarse_copy(f).wait_send)
        for copy in edge_copies(f):
            guard(dy, copy.wait_send)
    for copy in results:
        copy.wait()


def gradient_kernel(alpha, perts, ph, pw, pe, res, edge, lon, lat, inc, grad_out, inc_out):
    mask_a, mask_b = half_masks()
    mask_a, mask_b = mask_a.astype(F32), mask_b.astype(F32)
    inc_out[...] = inc[...]
    for level in range(2):
        west_b, east_b = pw[0].astype(F32), pe[0].astype(F32)
        edges = west_b * mask_a + east_b * mask_b if level == 0 else east_b * mask_a + west_b * mask_b
        edge_high, edge_low = split(edges * edge[level])
        for pair in range(GROUP // 2):
            stacks = []
            for j in (2 * pair, 2 * pair + 1):
                own = jnp.concatenate([perts[j, level], ph[j, level]], axis=0).astype(F32) * res[level]
                high, low = split(own)
                keep = image_mask(level, j)
                wide = dot(jnp.concatenate([high, edge_high * keep], axis=1), lon[level])
                thin = dot(jnp.concatenate([low, edge_low * keep], axis=1), lon[level, :, :TILE])
                stacks.append(lat_stack(wide[:, :TILE] + wide[:, TILE:] + thin))
            z = dot(lat[level], jnp.concatenate(stacks, axis=1))
            j = 2 * pair
            grad_out[j, level] = alpha[j, level].astype(F32) + z[:, :TILE]
            grad_out[j + 1, level] = alpha[j + 1, level].astype(F32) + z[:, TILE:]


def body(alpha, perts, widths, lat_index, lat_weight, lon_index, lon_weight, innovation, obs_weight):
    members = alpha.shape[0]
    chunks = members // GROUP
    any_space = pl.BlockSpec(memory_space=pl.ANY)
    vmem = pl.BlockSpec(memory_space=pltpu.VMEM)
    smem = pl.BlockSpec(memory_space=pltpu.SMEM)
    dma = pltpu.SemaphoreType.DMA
    shapes = [
        jax.ShapeDtypeStruct((2, FINE, FINE), F32),
        jax.ShapeDtypeStruct((2, EXT, TILE), F32),
        jax.ShapeDtypeStruct((2, EXT, TILE), F32),
        jax.ShapeDtypeStruct((members, 2, 16, TILE), BF16),
        jax.ShapeDtypeStruct((chunks, EXT, TILE), BF16),
        jax.ShapeDtypeStruct((chunks, EXT, TILE), BF16),
        jax.ShapeDtypeStruct((2, FINE, FINE), BF16),
        jax.ShapeDtypeStruct((2, TILE, 512), BF16),
    ]
    inc, res, edge, ph, pw, pe, lon, lat = pl.pallas_call(
        sum_kernel,
        out_shape=shapes,
        in_specs=[any_space, any_space, smem, vmem, vmem, vmem, vmem, any_space, any_space],
        out_specs=[any_space, vmem, vmem, any_space, any_space, any_space, vmem, vmem],
        scratch_shapes=[
            pltpu.VMEM(alpha.shape, BF16),
            pltpu.VMEM(alpha.shape, BF16),
            pltpu.VMEM((members, 2, 16, TILE), BF16),
            pltpu.VMEM((members, 2, 16, TILE), BF16),
            pltpu.VMEM((GROUP, FINE, FINE), BF16),
            pltpu.VMEM((2, chunks, TILE, TILE), BF16),
            pltpu.VMEM((2, chunks, TILE, TILE), BF16),
            pltpu.VMEM((chunks, TILE, TILE), BF16),
            pltpu.VMEM((chunks, TILE, TILE), BF16),
            pltpu.VMEM((chunks, EXT, TILE), BF16),
            pltpu.VMEM((chunks, EXT, TILE), BF16),
            pltpu.VMEM((chunks, 16, TILE), BF16),
            pltpu.VMEM((chunks, 16, TILE), BF16),
            pltpu.VMEM((2, TILE, TILE), F32),
            pltpu.VMEM((2, TILE, TILE), F32),
            pltpu.VMEM((2, TILE, TILE), F32),
            pltpu.VMEM((2, 2, HB, TILE), F32),
            pltpu.VMEM((8, 2, HB, TILE), F32),
            pltpu.VMEM((2, FINE, FINE), F32),
            pltpu.VMEM((2, FINE, FINE), F32),
            pltpu.VMEM((2, FINE, FINE), F32),
            pltpu.VMEM((2, EXT, TILE), F32),
            pltpu.VMEM((3, 2, 16, FINE), F32),
            pltpu.VMEM((2, 2, 16, TILE), F32),
            pltpu.VMEM((2, 2, 16, TILE), F32),
            pltpu.VMEM((8, 2, 16, FINE), F32),
            dma((3, chunks)),
            dma((8, chunks)), dma((8, chunks)), dma((8, chunks)), dma((8, chunks)),
            dma((2,)), dma((2,)), dma((8,)), dma((8,)), dma((10,)), dma((10,)), dma((4,)),
        ],
        compiler_params=pltpu.CompilerParams(
            collective_id=0, has_side_effects=True, vmem_limit_bytes=48 * 2**20),
        name="sum_kernel",
    )(
        alpha, perts, widths, lat_index[None], lat_weight[None], lon_index[None], lon_weight[None],
        innovation, obs_weight,
    )
    group = pl.BlockSpec((GROUP, 2, TILE, TILE), lambda b: (b, 0, 0, 0))
    block = pl.BlockSpec((1, EXT, TILE), lambda b: (b, 0, 0))

    def whole(x):
        return pl.BlockSpec(x.shape, lambda b: (0, 0, 0))

    gradient, increment = pl.pallas_call(
        gradient_kernel,
        grid=(chunks,),
        out_shape=[
            jax.ShapeDtypeStruct(alpha.shape, F32),
            jax.ShapeDtypeStruct((2, FINE, FINE), F32),
        ],
        in_specs=[
            group, group, pl.BlockSpec((GROUP, 2, 16, TILE), lambda b: (b, 0, 0, 0)),
            block, block, whole(res), whole(edge), whole(lon), whole(lat), whole(inc),
        ],
        out_specs=[group, whole(inc)],
        compiler_params=pltpu.CompilerParams(
            dimension_semantics=("arbitrary",), vmem_limit_bytes=48 * 2**20),
        name="gradient_kernel",
    )(alpha, perts, ph, pw, pe, res, edge, lon, lat, inc)
    return (increment, gradient)


def solution(mesh):
    placed = (
        P("ma", None, "gy", "gx"),
        P("ma", None, "gy", "gx"),
        P(),
        P("gy"),
        P("gy"),
        P("gx"),
        P("gx"),
        P(None, "gy", "gx"),
        P(None, "gy", "gx"),
    )
    return jax.shard_map(
        body,
        mesh=mesh,
        in_specs=placed,
        out_specs=(P(None, "gy", "gx"), P("ma", None, "gy", "gx")),
        check_vma=False,
    )
```

```python
import functools

import jax
import jax.numpy as jnp
from jax import lax
from jax.experimental import pallas as pl
from jax.experimental.pallas import tpu as pltpu
from jax.sharding import PartitionSpec as P

HB = 8
TILE = 128
EXT = 144
FINE = 256
GROUP = 8
F32 = jnp.float32
BF16 = jnp.bfloat16
MESH = pl.DeviceIdType.MESH
FLOWS = ((1, 0), (-1, 0), (0, 1), (0, -1), (1, 1), (1, -1), (-1, 1), (-1, -1))


def iota(shape, dim):
    return lax.broadcasted_iota(jnp.int32, shape, dim)


def dot(a, b):
    return jnp.dot(a, b, preferred_element_type=F32)


def split(x):
    high = x.astype(BF16)
    return high, (x - high.astype(F32)).astype(BF16)


def dot3(a, b):
    return dot(a[0], b[0]) + dot(a[0], b[1]) + dot(a[1], b[0])


def taps_at(distance, width):
    spread = jnp.full((8, 128), width.astype(F32), F32)[:1]
    scale = 1.0 / (2.0 * spread * spread)
    offset = (iota((1, 128), 1) - HB).astype(F32)
    shape = jnp.where(iota((1, 128), 1) <= 2 * HB, jnp.exp(-offset * offset * scale), 0.0)
    norm = 1.0 / jnp.sqrt(jnp.sum(shape * shape, axis=1, keepdims=True))
    gap = distance.astype(F32)
    values = jnp.exp(-gap * gap * scale[:, :1]) * norm
    return jnp.where(jnp.abs(distance) <= HB, values, 0.0)


def lon_taps(level, width):
    row = iota((2 * TILE, TILE), 0)
    col = iota((2 * TILE, TILE), 1)
    first = (row & 15) < 8
    west = first if level == 0 else jnp.logical_not(first)
    place = jnp.where(row < TILE, row, jnp.where(west, (row & 7) - HB, TILE + (row & 7)))
    high, low = split(taps_at(place - col, width))
    return jnp.concatenate([
        jnp.concatenate([high, low], axis=1), jnp.concatenate([high, jnp.zeros_like(high)], axis=1)], axis=0)


def lat_taps(width):
    row = iota((TILE, 512), 0)
    col = iota((TILE, 512), 1)
    part = (col >= EXT).astype(jnp.int32) + (col >= 2 * EXT).astype(jnp.int32) + (col >= 3 * EXT).astype(jnp.int32)
    k = col - EXT * part
    place = jnp.where(k < TILE, k, jnp.where(k < TILE + HB, k - TILE - HB, k - HB))
    values = taps_at(place - row, width)
    high = values.astype(BF16).astype(F32)
    chosen = jnp.where(part == 2, values - high, jnp.where(part == 3, 0.0, high))
    return chosen.astype(BF16)


def stencil_t(relative, weight):
    cell = iota((FINE, FINE), 0)

    def ext(r):
        return jnp.where(r < 0, r + EXT - HB, jnp.where(r >= TILE, r + HB, r))

    near = jnp.where(cell == ext(relative), 1.0 - weight, 0.0)
    return near + jnp.where(cell == ext(relative + 1), weight, 0.0)


def image_mask(level, j):
    lane = iota((1, TILE), 1)
    start = (lane - 16 * j + (8 if level == 1 else 0)) & 127
    return jnp.where(start < 16, 1.0, 0.0).astype(BF16)


def half_masks():
    lane = iota((1, TILE), 1)
    first = jnp.where((lane & 15) < 8, 1.0, 0.0)
    return first.astype(BF16), (1.0 - first).astype(BF16)


def keep_stack(stack, i, y):
    high, low = split(y)
    for k, part in enumerate((high, low, high)):
        stack[k * EXT:(k + 1) * EXT, i * TILE:(i + 1) * TILE] = part


def sum_kernel(
    alpha_hbm, perts_hbm, width_hbm, lat_i_hbm, lat_w_hbm, lon_i_hbm, lon_w_hbm, innov_hbm, weight_hbm,
    inc, res_out, edge_out, ph_out, pw_out, pe_out, lon_out, lat_out, alpha, perts,
    ah, ph, pick, apk, ppk, aw, ae, pw, pe, awh, aeh, stack,
    acc, other, coarse, ce, hc, innov, wobs, resm, sel, rows, hm, hs,
    width_ref, lat_i, lat_w, lon_i, lon_w, mt2, m2, nt2, n2, corner2, place,
    load_sem, a_send, a_recv, p_send, p_recv, m_send, m_recv, c_send, c_recv, r_send, r_recv,
):
    gx, gy, ma = lax.axis_index("gx"), lax.axis_index("gy"), lax.axis_index("ma")
    nx, ny = lax.axis_size("gx"), lax.axis_size("gy")
    chunks = alpha.shape[0] // GROUP
    east, west = lax.rem(gx + 1, nx), lax.rem(gx + nx - 1, nx)
    has_up, has_down = gy > 0, gy < ny - 1

    def device(dx, dy):
        return (gx if dx == 0 else (east if dx == 1 else west), gy + dy, ma)

    def guard(dy, body):
        if dy == 0:
            body()
        else:
            pl.when(has_down if dy == 1 else has_up)(body)

    def load(i, b):
        src, dst = ((alpha_hbm, alpha), (perts_hbm, perts))[i]
        rows = pl.ds(b * GROUP, GROUP)
        return pltpu.make_async_copy(src.at[rows], dst.at[rows], load_sem.at[i, b])

    for i in range(2):
        for b in range(chunks):
            load(i, b).start()
    small_loads = [
        pltpu.make_async_copy(src, dst, load_sem.at[3, k])
        for k, (src, dst) in enumerate((
            (lat_i_hbm, lat_i), (lat_w_hbm, lat_w), (lon_i_hbm, lon_i), (lon_w_hbm, lon_w)))
    ]
    width_load = pltpu.make_async_copy(width_hbm, width_ref, load_sem.at[2, 2])
    for copy in (*small_loads, width_load):
        copy.start()
    fine_loads = [
        pltpu.make_async_copy(innov_hbm, innov, load_sem.at[2, 0]),
        pltpu.make_async_copy(weight_hbm, wobs, load_sem.at[2, 1]),
    ]
    for copy in fine_loads:
        copy.start()

    barrier = pltpu.get_barrier_semaphore()
    for dx, dy in FLOWS:
        guard(dy, functools.partial(
            pl.semaphore_signal, barrier, inc=1, device_id=device(dx, dy), device_id_type=MESH))
    partner = (gx, gy, 1 - ma)
    pl.semaphore_signal(barrier, inc=1, device_id=partner, device_id_type=MESH)

    row = iota((2 * TILE, 2 * TILE), 0)
    col = iota((2 * TILE, 2 * TILE), 1)
    lane, lev = col & 127, row >> 7
    src = row & 127
    for j in range(GROUP):
        target_e = (16 * j - 8 * lev + src - 120) & 127
        target_w = (16 * j + 8 - 8 * lev + src) & 127
        hit = jnp.where(
            col < TILE,
            jnp.where(src >= 120, (lane == target_e).astype(jnp.int32), 0),
            jnp.where(src < 8, (lane == target_w).astype(jnp.int32), 0),
        )
        pick[j] = hit.astype(F32).astype(BF16)

    def pack(i, fields, packed):
        def one(b, carry):
            load(i, b).wait()
            total = jnp.zeros((TILE, 2 * TILE), F32)
            for j in range(GROUP):
                m = b * GROUP + j
                total = total + dot(jnp.concatenate([fields[m, 0], fields[m, 1]], axis=1), pick[j])
            packed[0, b] = total[:, :TILE].astype(BF16)
            packed[1, b] = total[:, TILE:].astype(BF16)
            return carry

        lax.fori_loop(0, chunks, one, 0)

    def band_copy(f, b, fields, packed, rows_halo, blocks, block_rows, send, recv):
        dx, dy = FLOWS[f]
        edge = pl.ds(TILE - HB, HB) if dy == 1 else pl.ds(0, HB)
        land = pl.ds(0, HB) if dy == 1 else pl.ds(HB, HB)
        members = pl.ds(b * GROUP, GROUP)
        if dx == 0:
            src, dst = fields.at[members, :, edge], rows_halo.at[members, :, land]
        elif dy == 0:
            src, dst = packed.at[0 if dx == 1 else 1, b], blocks[0 if dx == 1 else 1].at[b]
        else:
            src = packed.at[0 if dx == 1 else 1, b, edge]
            dst = block_rows[0 if dx == 1 else 1].at[b, land]
        return pltpu.make_async_remote_copy(
            src_ref=src, dst_ref=dst, send_sem=send.at[f, b], recv_sem=recv.at[f, b],
            device_id=device(dx, dy), device_id_type=MESH)

    a_args = (alpha, apk, ah, (aw, ae), (awh, aeh), a_send, a_recv)
    p_args = (perts, ppk, ph, (pw.at[:, pl.ds(0, TILE)], pe.at[:, pl.ds(0, TILE)]),
              (pw.at[:, pl.ds(TILE, 16)], pe.at[:, pl.ds(TILE, 16)]), p_send, p_recv)

    def each_band(action, args):
        def one(b, carry):
            for f, (dx, dy) in enumerate(FLOWS):
                copy = band_copy(f, b, *args)
                if action == "start":
                    guard(dy, copy.start)
                elif action == "send":
                    guard(dy, copy.wait_send)
                else:
                    guard(-dy, copy.wait_recv)
            return carry

        lax.fori_loop(0, chunks, one, 0)

    pack(0, alpha, apk)
    pl.semaphore_wait(
        barrier, 3 + 3 * has_up.astype(jnp.int32) + 3 * has_down.astype(jnp.int32))
    each_band("start", a_args)

    def clear(first):
        land = pl.ds(0, HB) if first else pl.ds(HB, HB)
        far = pl.ds(TILE, HB) if first else pl.ds(TILE + HB, HB)
        ah[:, :, land] = jnp.zeros((ah.shape[0], 2, HB, TILE), BF16)
        ph[:, :, land] = jnp.zeros((ah.shape[0], 2, HB, TILE), BF16)
        for block in (awh, aeh):
            block[:, land] = jnp.zeros((chunks, HB, TILE), BF16)
        for block in (pw, pe):
            block[:, far] = jnp.zeros((chunks, HB, TILE), BF16)
        dy = 1 if first else -1
        for f, flow in enumerate(FLOWS):
            if flow[1] == dy:
                hc[f] = jnp.zeros((2, HB, TILE), F32)
                hs[f] = jnp.zeros((2, 16, FINE), F32)
        hm[0 if first else 1] = jnp.zeros((2, 16, TILE), F32)

    pl.when(gy == 0)(functools.partial(clear, True))
    pl.when(gy == ny - 1)(functools.partial(clear, False))

    stack[:, 3 * EXT:] = jnp.zeros((2, 512 - 3 * EXT, GROUP * TILE), BF16)
    width_load.wait()
    for level in range(2):
        lon_out[level] = lon_taps(level, width_ref[level])
        lat_out[level] = lat_taps(width_ref[level])

    pack(1, perts, ppk)
    each_band("start", p_args)

    for copy in small_loads:
        copy.wait()
    lat_rel = lat_i[...] - gy * TILE
    lon_rel = lax.rem(lon_i[...] - gx * TILE + 1 + nx * TILE, nx * TILE) - 1
    mt = stencil_t(lat_rel, lat_w[...])
    nt = stencil_t(lon_rel, lon_w[...])
    zeros_top = jnp.zeros((TILE - HB, FINE), F32)
    top_t = jnp.concatenate([zeros_top, mt[TILE:TILE + HB]], axis=0)
    bottom_t = jnp.concatenate([mt[TILE + HB:EXT], zeros_top], axis=0)
    corner = jnp.concatenate([mt[:TILE], top_t, bottom_t], axis=0)
    for table, value in ((mt2, mt), (m2, mt.T), (nt2, nt), (n2, nt.T), (corner2, corner)):
        table[0], table[1] = split(value)
    r = iota((TILE, FINE), 0)
    c = iota((TILE, FINE), 1)
    for level in range(2):
        band = (c & 15) if level == 0 else (c & 15) ^ 8
        own = jnp.where(c < HB, c + 16, jnp.where(c >= TILE - HB, c - 96, -1))
        place[level] = jnp.where(r == jnp.where(c < TILE, own, band), 1.0, 0.0).astype(BF16)

    mask_a, mask_b = half_masks()

    def partner_copy(level):
        return pltpu.make_async_remote_copy(
            src_ref=acc.at[level], dst_ref=other.at[level], send_sem=m_send.at[level],
            recv_sem=m_recv.at[level], device_id=partner, device_id_type=MESH)

    def add_chunk(b, level):
        west_b = jnp.concatenate([aw[b], awh[b]], axis=0)
        east_b = jnp.concatenate([ae[b], aeh[b]], axis=0)
        edges = west_b * mask_a + east_b * mask_b if level == 0 else east_b * mask_a + west_b * mask_b
        for j in range(GROUP):
            m = b * GROUP + j
            own = jnp.concatenate([alpha[m, level], ah[m, level]], axis=0)
            lhs = jnp.concatenate([own, edges * image_mask(level, j)], axis=1)
            wide = dot(lhs, lon_out[level, :2 * TILE])
            keep_stack(stack.at[level], j, wide[:, :TILE] + wide[:, TILE:])
        total = acc[level]
        for pair in range(GROUP // 2):
            z = dot(lat_out[level], stack[level, :, pair * FINE:(pair + 1) * FINE])
            m = b * GROUP + 2 * pair
            total = total + perts[m, level].astype(F32) * z[:, :TILE]
            total = total + perts[m + 1, level].astype(F32) * z[:, TILE:]
        acc[level] = total

    def arrive(b):
        for f, (dx, dy) in enumerate(FLOWS):
            guard(-dy, band_copy(f, b, *a_args).wait_recv)

    def chunk(b, carry):
        arrive(b)
        for level in range(2):
            add_chunk(b, level)
        return carry

    acc[...] = jnp.zeros((2, TILE, TILE), F32)
    lax.fori_loop(0, chunks - 1, chunk, 0)
    arrive(chunks - 1)
    for level in range(2):
        add_chunk(chunks - 1, level)
        partner_copy(level).start()

    def coarse_copy(f, level):
        dx, dy = FLOWS[f]
        edge = pl.ds(TILE - HB, HB) if dy == 1 else pl.ds(0, HB)
        src = coarse.at[level, edge] if dx == 0 else ce.at[0 if dx == 1 else 1, level]
        return pltpu.make_async_remote_copy(
            src_ref=src, dst_ref=hc.at[f, level], send_sem=c_send.at[f, level],
            recv_sem=c_recv.at[f, level], device_id=device(dx, dy), device_id_type=MESH)

    def edge_copies(f, level):
        dx, dy = FLOWS[f]
        copies = [pltpu.make_async_remote_copy(
            src_ref=sel.at[2 if dx == 0 else (0 if dx == 1 else 1), level], dst_ref=hs.at[f, level],
            send_sem=r_send.at[f, level], recv_sem=r_recv.at[f, level],
            device_id=device(dx, dy), device_id_type=MESH)]
        if dx == 0:
            k = 0 if dy == 1 else 1
            copies.append(pltpu.make_async_remote_copy(
                src_ref=rows.at[k, level], dst_ref=hm.at[k, level], send_sem=r_send.at[8 + k, level],
                recv_sem=r_recv.at[8 + k, level], device_id=device(dx, dy), device_id_type=MESH))
        return copies

    def total_step(level):
        partner_copy(level).wait_recv()
        total = acc[level] + other[level]
        coarse[level] = total
        turned = total.T
        ce[0, level] = turned[TILE - HB:]
        ce[1, level] = turned[:HB]
        for f, (dx, dy) in enumerate(FLOWS):
            guard(dy, coarse_copy(f, level).start)

    def fine_step(level):
        for f, (dx, dy) in enumerate(FLOWS):
            guard(-dy, coarse_copy(f, level).wait_recv)
        framed = jnp.concatenate(
            [coarse[level], hc[2, level], hc[3, level], jnp.zeros((FINE - EXT, TILE), F32)], axis=0)
        by_lat = dot3(m2, split(framed))
        sides = jnp.concatenate([
            jnp.concatenate([hc[0, level], hc[1, level]], axis=0),
            jnp.concatenate([hc[4, level], hc[6, level]], axis=0),
            jnp.concatenate([hc[5, level], hc[7, level]], axis=0)], axis=1)
        side_t = dot3(split(sides), corner2)
        side = jnp.concatenate([side_t, jnp.zeros((TILE - 16, FINE), F32)], axis=0).T
        fine = dot3(split(jnp.concatenate([by_lat, side], axis=1)), nt2)
        inc[level] = fine
        misfit = split(wobs[level] * (fine - innov[level]))
        lon_back = split(dot3(misfit, (n2[0, :, :TILE], n2[1, :, :TILE])))

        def turned_dot(part, values):
            table = jnp.concatenate([
                part[:HB], part[TILE:TILE + HB], part[TILE - HB:TILE], part[TILE + HB:EXT]], axis=0)
            return lax.dot_general(
                table.astype(BF16), values, (((1,), (1,)), ((), ())), preferred_element_type=F32)

        high, low = nt2[0].astype(F32), nt2[1].astype(F32)
        chosen_t = turned_dot(high, misfit[0]) + turned_dot(high, misfit[1]) + turned_dot(low, misfit[0])
        restricted = dot3((mt2[0, :EXT], mt2[1, :EXT]), lon_back)
        resm[level] = restricted
        turned = dot3(split(chosen_t), m2)
        sel[0, level] = turned[16:32]
        sel[1, level] = turned[:16]
        sel[2, level] = jnp.concatenate([turned[8:16], turned[24:32]], axis=0)
        rows[0, level] = jnp.concatenate([restricted[TILE - HB:TILE], restricted[TILE + HB:EXT]], axis=0)
        rows[1, level] = jnp.concatenate([restricted[:HB], restricted[TILE:TILE + HB]], axis=0)
        for f, (dx, dy) in enumerate(FLOWS):
            for copy in edge_copies(f, level):
                guard(dy, copy.start)

    lane = iota((32, FINE), 1)

    def joined(from_west, centre, from_east):
        halo = centre + jnp.concatenate([from_west[:HB], from_east[:HB]], axis=0)
        return jnp.concatenate([halo, from_west[HB:], from_east[HB:]], axis=0)

    def pick_lanes(x, first, first_shift, second, second_shift):
        a = pltpu.roll(x, first_shift, 1)
        b = pltpu.roll(x, second_shift, 1)
        in_a = (lane >= first) & (lane < first + HB)
        in_b = (lane >= second) & (lane < second + HB)
        return jnp.where(in_a, a, jnp.where(in_b, b, 0.0))

    def residual_step(level):
        for f, (dx, dy) in enumerate(FLOWS):
            for copy in edge_copies(f, level):
                guard(-dy, copy.wait_recv)
        side = joined(hs[0, level], sel[2, level], hs[1, level])
        above = joined(hs[4, level], hs[2, level], hs[6, level])
        below = joined(hs[5, level], hs[3, level], hs[7, level])
        side = side + pick_lanes(above, TILE, 8, 0, 120)
        side = side + pick_lanes(below, TILE + HB, 136, TILE - HB, 248)
        turned = split(jnp.concatenate([side, jnp.zeros((TILE - 32, FINE), F32)], axis=0).T)
        spread = dot(turned[0], place[level]) + dot(turned[1], place[level])
        edge_out[level] = spread[:EXT, TILE:]
        top, bottom = hm[0, level], hm[1, level]
        gap = jnp.zeros((TILE - 2 * HB, TILE), F32)
        arrived = jnp.concatenate([top[HB:], gap, bottom[HB:], top[:HB], bottom[:HB]], axis=0)
        res_out[level] = resm[level] + spread[:EXT, :TILE] + arrived

    total_step(0)
    total_step(1)
    for copy in fine_loads:
        copy.wait()
    fine_step(0)
    fine_step(1)
    each_band("recv", p_args)
    ph_out[...] = ph[...]
    pw_out[...] = pw[...]
    pe_out[...] = pe[...]
    residual_step(0)
    residual_step(1)
    each_band("send", a_args)
    each_band("send", p_args)
    for level in range(2):
        partner_copy(level).wait_send()
        for f, (dx, dy) in enumerate(FLOWS):
            guard(dy, coarse_copy(f, level).wait_send)
            for copy in edge_copies(f, level):
                guard(dy, copy.wait_send)


def gradient_kernel(
    alpha, perts, ph, pw, pe, res, edge, lon, lat, inc, grad_out, inc_out, lhs, stack, result, grad_sem, inc_sem,
):
    inc_copy = pltpu.make_async_copy(inc, inc_out, inc_sem)
    inc_copy.start()
    mask_a, mask_b = (mask.astype(F32) for mask in half_masks())
    stack[:, 3 * EXT:] = jnp.zeros((2, 512 - 3 * EXT, GROUP * TILE), BF16)

    def out_copy(b, level):
        members = pl.ds(b * GROUP, GROUP)
        return pltpu.make_async_copy(
            result.at[members, level], grad_out.at[members, level], grad_sem.at[level, b])

    def chunk(b, carry):
        west_b, east_b = pw[b].astype(F32), pe[b].astype(F32)
        for level in range(2):
            edges = west_b * mask_a + east_b * mask_b if level == 0 else east_b * mask_a + west_b * mask_b
            edge_high, edge_low = split(edges * edge[level])
            for j in range(GROUP):
                m = b * GROUP + j
                own = jnp.concatenate([perts[m, level], ph[m, level]], axis=0).astype(F32) * res[level]
                high, low = split(own)
                keep = image_mask(level, j)
                for k, part in enumerate((high, edge_high * keep, low, edge_low * keep)):
                    lhs[level, j * EXT:(j + 1) * EXT, k * TILE:(k + 1) * TILE] = part
            for j in range(GROUP):
                wide = dot(lhs[level, j * EXT:(j + 1) * EXT], lon[level])
                keep_stack(stack.at[level], j, wide[:, :TILE] + wide[:, TILE:])
            for pair in range(GROUP // 2):
                z = dot(lat[level], stack[level, :, pair * FINE:(pair + 1) * FINE])
                m = b * GROUP + 2 * pair
                result[m, level] = alpha[m, level].astype(F32) + z[:, :TILE]
                result[m + 1, level] = alpha[m + 1, level].astype(F32) + z[:, TILE:]
            out_copy(b, level).start()
        return carry

    chunks = pw.shape[0]
    lax.fori_loop(0, chunks, chunk, 0)
    for b in range(chunks):
        for level in range(2):
            out_copy(b, level).wait()
    inc_copy.wait()


def body(alpha, perts, widths, lat_index, lat_weight, lon_index, lon_weight, innovation, obs_weight):
    members = alpha.shape[0]
    chunks = members // GROUP
    hbm = pl.BlockSpec(memory_space=pltpu.HBM)
    vmem = pl.BlockSpec(memory_space=pltpu.VMEM)
    dma = pltpu.SemaphoreType.DMA
    fine = (2, FINE, FINE)
    shapes = [
        pltpu.VMEM(fine, F32),
        pltpu.VMEM((2, EXT, TILE), F32),
        pltpu.VMEM((2, EXT, TILE), F32),
        pltpu.VMEM((members, 2, 16, TILE), BF16),
        pltpu.VMEM((chunks, EXT, TILE), BF16),
        pltpu.VMEM((chunks, EXT, TILE), BF16),
        pltpu.VMEM((2, 2 * FINE, FINE), BF16),
        pltpu.VMEM((2, TILE, 2 * FINE), BF16),
        pltpu.VMEM(alpha.shape, BF16),
        pltpu.VMEM(alpha.shape, BF16),
    ]
    inc, res, edge, ph, pw, pe, lon, lat, alpha_v, perts_v = pl.pallas_call(
        sum_kernel,
        out_shape=shapes,
        in_specs=[hbm] * 9,
        out_specs=[vmem] * len(shapes),
        scratch_shapes=[
            pltpu.VMEM((members, 2, 16, TILE), BF16),
            pltpu.VMEM((members, 2, 16, TILE), BF16),
            pltpu.VMEM((GROUP, FINE, FINE), BF16),
            pltpu.VMEM((2, chunks, TILE, TILE), BF16),
            pltpu.VMEM((2, chunks, TILE, TILE), BF16),
            pltpu.VMEM((chunks, TILE, TILE), BF16),
            pltpu.VMEM((chunks, TILE, TILE), BF16),
            pltpu.VMEM((chunks, EXT, TILE), BF16),
            pltpu.VMEM((chunks, EXT, TILE), BF16),
            pltpu.VMEM((chunks, 16, TILE), BF16),
            pltpu.VMEM((chunks, 16, TILE), BF16),
            pltpu.VMEM((2, 2 * FINE, GROUP * TILE), BF16),
            pltpu.VMEM((2, TILE, TILE), F32),
            pltpu.VMEM((2, TILE, TILE), F32),
            pltpu.VMEM((2, TILE, TILE), F32),
            pltpu.VMEM((2, 2, HB, TILE), F32),
            pltpu.VMEM((8, 2, HB, TILE), F32),
            pltpu.VMEM(fine, F32),
            pltpu.VMEM(fine, F32),
            pltpu.VMEM((2, EXT, TILE), F32),
            pltpu.VMEM((3, 2, 16, FINE), F32),
            pltpu.VMEM((2, 2, 16, TILE), F32),
            pltpu.VMEM((2, 2, 16, TILE), F32),
            pltpu.VMEM((8, 2, 16, FINE), F32),
            pltpu.SMEM((2,), jnp.int32),
            pltpu.VMEM((1, FINE), jnp.int32),
            pltpu.VMEM((1, FINE), F32),
            pltpu.VMEM((1, FINE), jnp.int32),
            pltpu.VMEM((1, FINE), F32),
            pltpu.VMEM(fine, BF16),
            pltpu.VMEM(fine, BF16),
            pltpu.VMEM(fine, BF16),
            pltpu.VMEM(fine, BF16),
            pltpu.VMEM((2, 3 * TILE, FINE), BF16),
            pltpu.VMEM((2, TILE, FINE), BF16),
            dma((4, chunks)),
            dma((8, chunks)), dma((8, chunks)), dma((8, chunks)), dma((8, chunks)),
            dma((2,)), dma((2,)), dma((8, 2)), dma((8, 2)), dma((10, 2)), dma((10, 2)),
        ],
        compiler_params=pltpu.CompilerParams(
            collective_id=0, has_side_effects=True, vmem_limit_bytes=32 * 2**20),
        name="sum_kernel",
    )(*(pltpu.with_memory_space_constraint(x, pltpu.HBM) for x in (
        alpha, perts, widths, lat_index[None], lat_weight[None], lon_index[None], lon_weight[None],
        innovation, obs_weight)))
    gradient, increment = pl.pallas_call(
        gradient_kernel,
        out_shape=[
            jax.ShapeDtypeStruct(alpha.shape, F32),
            jax.ShapeDtypeStruct(fine, F32),
        ],
        in_specs=[vmem] * 10,
        out_specs=[hbm, hbm],
        scratch_shapes=[
            pltpu.VMEM((2, GROUP * EXT, 2 * FINE), BF16),
            pltpu.VMEM((2, 2 * FINE, GROUP * TILE), BF16),
            pltpu.VMEM(alpha.shape, F32),
            dma((2, chunks)), dma,
        ],
        compiler_params=pltpu.CompilerParams(vmem_limit_bytes=32 * 2**20),
        name="gradient_kernel",
    )(alpha_v, perts_v, ph, pw, pe, res, edge, lon, lat, inc)
    return (increment, gradient)


def solution(mesh):
    placed = (
        P("ma", None, "gy", "gx"),
        P("ma", None, "gy", "gx"),
        P(),
        P("gy"),
        P("gy"),
        P("gx"),
        P("gx"),
        P(None, "gy", "gx"),
        P(None, "gy", "gx"),
    )
    return jax.shard_map(
        body,
        mesh=mesh,
        in_specs=placed,
        out_specs=(P(None, "gy", "gx"), P("ma", None, "gy", "gx")),
        check_vma=False,
    )
```
